32 devices in a mesh: row: 8 (over z, core), col: 4 (over y, x).
Axes of the slice: x: 2, y: 2, z: 4, core: 2. Of those that a mesh axis runs over, the one named last changes fastest.
Arguments:
- ladder_ints: float32 [4928, 4928], P('row', 'col'), may hold values from -0.078125 to 0.078125
- amplitudes: float32 [4928, 1024], P('row', 'col'), may hold values from -6 to 6
- phase_map: int32 [8], replicated, may hold values from 0 to 7, each once
Outputs:
- ladder_term: float32 [4928, 1024], P('row', 'col')
The draws below stay inside these ranges and needn't reach their ends.
Inputs may be any that keep to these rules, and one draw needn't show every extreme that they name: `phase_map`: each phase appears once.
All inputs are finite; a program needn't handle non-finite values.
Results may differ from the reference program's by a relative error of at most 0.000078.
Values sent between devices are 32-bit elements; how exact they have to be, the bound alone decides.
No kernel may reach another device: no remote copies, remote signals or barrier semaphores. Data moves between devices by JAX's collectives and lax.ppermute only.
A program may use at most 320 MiB of HBM per device.

```python
import jax
import jax.numpy as jnp
from jax import lax

PAIRS = 4928
OCC_PAIRS = 1024
PHASES = 8
N_ROW = 8


def shard_levels(own_key, extent, shards, low, top_value):
    factor_of, own = 1.0, jax.random.fold_in(own_key, 6)
    for axis_at, shards_of in shards:
        draws = jnp.exp(jax.random.uniform(jax.random.fold_in(own, axis_at), (shards_of,), jnp.float32, low / len(shards), top_value / len(shards)))
        factor_of = factor_of * jnp.repeat(draws, extent[axis_at] // shards_of).reshape([-1 if axis == axis_at else 1 for axis in range(len(extent))])
    return factor_of


def gaussian(key, dims, scale, limit, split=(), kind=jnp.bfloat16):
    array = jax.random.normal(key, dims, jnp.float32) * scale
    if len(split) > 0:
        array = shard_levels(key, dims, split, -0.22, 0.18) * array
    return jnp.clip(array, min=-limit, max=limit).astype(kind)


def setup_inputs(seed: int = 0) -> dict:
    streams_of = jax.random.split(jax.random.key(seed), 4)
    ladder_ints = gaussian(streams_of[0], (PAIRS, PAIRS), PAIRS ** -0.5, 0.078125, ((0, 8), (1, 4)), jnp.float32)
    amplitudes = gaussian(streams_of[1], (PAIRS, OCC_PAIRS), 1.0, 6.0, ((0, 8), (1, 4)), jnp.float32)
    phase_map = jax.random.permutation(streams_of[2], N_ROW).astype(jnp.int32)
    return {"ladder_ints": ladder_ints, "amplitudes": amplitudes, "phase_map": phase_map}


def reference(ladder_ints, amplitudes, phase_map):
    block = PAIRS // PHASES
    inverse = jnp.zeros((PHASES,), jnp.int32).at[phase_map.astype(jnp.int32)].set(jnp.arange(PHASES, dtype=jnp.int32))
    shaped = amplitudes.reshape(PHASES, block, OCC_PAIRS)
    by_phase = jnp.take(shaped, inverse, axis=0)
    ordered = jnp.transpose(by_phase, (1, 0, 2)).reshape(PAIRS, OCC_PAIRS)
    return jnp.dot(ladder_ints, ordered, precision=lax.Precision.HIGHEST, preferred_element_type=jnp.float32)
```

```python
import functools

import jax
import jax.numpy as jnp
from jax import lax
from jax.experimental import pallas as pl
from jax.experimental.pallas import tpu as pltpu
from jax.sharding import PartitionSpec as P

TILE = 256


def ring_row(position, n):
    return jnp.where(position < n // 2, 2 * position, 2 * (n - 1 - position) + 1)


def ring_place(row, n):
    return jnp.where(row % 2 == 0, row // 2, n - 1 - row // 2)


def ring_pairs(n):
    order = list(range(0, n, 2)) + list(range(n - 1, 0, -2))
    forward = [(order[i], order[(i + 1) % n]) for i in range(n)]
    return forward, [(b, a) for a, b in forward]


def split(x):
    high = x.astype(jnp.bfloat16)
    low = (x - high.astype(jnp.float32)).astype(jnp.bfloat16)
    return high, low


def cut_kernel(cols, rows, source, *pieces):
    me = lax.axis_index("col")
    for piece in pieces:
        piece[rows:, :] = jnp.zeros((piece.shape[0] - rows, piece.shape[1]), jnp.float32)
    for own in range(cols):

        @pl.when(me == own)
        def _():
            for j, piece in enumerate(pieces):
                start = (own ^ j) * rows
                piece[:rows, :] = source[start : start + rows, :]


def cut(amplitudes, cols, rows, padded):
    width = amplitudes.shape[1]
    out = jax.ShapeDtypeStruct((padded, width), jnp.float32)
    return pl.pallas_call(
        functools.partial(cut_kernel, cols, rows),
        out_shape=[out] * cols,
        name="cut",
        cost_estimate=pl.CostEstimate(
            flops=amplitudes.size, bytes_accessed=8 * amplitudes.size, transcendentals=0
        ),
    )(amplitudes)


def order_kernel(phases, tiles, ints, high_out, low_out):
    group = TILE // phases
    into = lax.broadcasted_iota(jnp.int32, (TILE, TILE), 1)
    source = lax.broadcasted_iota(jnp.int32, (TILE, TILE), 0)
    wanted = (into % group) * phases + into // group
    pick = jnp.where(source == wanted, 1.0, 0.0).astype(jnp.bfloat16)
    total = ints.shape[1]
    for t in range(tiles):
        stop = min(TILE, total - t * TILE)
        high, low = split(ints[:, t * TILE : t * TILE + stop])
        chosen = pick[:stop, :]
        at = pl.ds(t * TILE, TILE)
        high_out[:, at] = jnp.dot(
            high, chosen, preferred_element_type=jnp.float32
        ).astype(jnp.bfloat16)
        low_out[:, at] = jnp.dot(
            low, chosen, preferred_element_type=jnp.float32
        ).astype(jnp.bfloat16)


def order(ints, phases, tiles):
    out = jax.ShapeDtypeStruct((ints.shape[0], tiles * TILE), jnp.bfloat16)
    return pl.pallas_call(
        functools.partial(order_kernel, phases, tiles),
        out_shape=[out, out],
        name="order",
        cost_estimate=pl.CostEstimate(
            flops=4 * ints.size * TILE, bytes_accessed=8 * ints.size, transcendentals=0
        ),
    )(ints)


def product_kernel(offsets, tiles, n_add, outs, phase_map, high, low, *refs):
    blocks = refs[: len(offsets)]
    adds = refs[len(offsets) : len(offsets) + len(n_add)]
    results = refs[len(offsets) + len(n_add) : len(offsets) + len(n_add) + len(outs)]
    t_high, t_low = refs[-2:]
    n = len(offsets)
    group = TILE // n
    place = ring_place(lax.axis_index("row"), n)
    for block, offset in zip(blocks, offsets):
        phase = phase_map[ring_row((place + offset + n) % n, n)]
        b_high, b_low = split(block[...])
        for t in range(tiles):
            at = pl.ds(pl.multiple_of(t * TILE + phase * group, group), group)
            t_high[at, :] = b_high[t * group : (t + 1) * group, :]
            t_low[at, :] = b_low[t * group : (t + 1) * group, :]
    total = jnp.dot(high[...], t_high[...], preferred_element_type=jnp.float32)
    total += jnp.dot(low[...], t_high[...], preferred_element_type=jnp.float32)
    total += jnp.dot(high[...], t_low[...], preferred_element_type=jnp.float32)
    parts = {}
    for result, (start, width) in zip(results, outs):
        value = total[:, start : start + width]
        for add, (first, size) in zip(adds, n_add):
            if first == start and size == width:
                value += add[...]
            elif start <= first and first + size <= start + width:
                parts.setdefault((start, width), []).append((add, first - start, size))
        result[...] = value
        for add, first, size in parts.get((start, width), []):
            result[:, first : first + size] += add[...]


def product(phase_map, high, low, blocks, offsets, tiles, adds, outs):
    rows, depth = high.shape
    width = blocks[0].shape[1]
    vmem = pl.BlockSpec(memory_space=pltpu.VMEM)
    spots = tuple((first, a.shape[1]) for a, first in adds)
    return pl.pallas_call(
        functools.partial(product_kernel, offsets, tiles, spots, outs),
        out_shape=[jax.ShapeDtypeStruct((rows, w), jnp.float32) for _, w in outs],
        in_specs=[pl.BlockSpec(memory_space=pltpu.SMEM)] + [vmem] * (2 + len(blocks) + len(adds)),
        scratch_shapes=[pltpu.VMEM((depth, width), jnp.bfloat16)] * 2,
        name="product",
        cost_estimate=pl.CostEstimate(
            flops=6 * rows * depth * width,
            bytes_accessed=4 * rows * depth + 4 * depth * width + 4 * rows * width,
            transcendentals=0,
        ),
    )(phase_map, high, low, *blocks, *[a for a, _ in adds])


def gather(chunk, n):
    forward, backward = ring_pairs(n)
    half = n // 2
    up, down = chunk, chunk
    found = [(0, chunk)]
    odd = {}
    for step in range(1, half):
        up = lax.ppermute(up, "row", forward)
        down = lax.ppermute(down, "row", backward)
        found += [(-step, up), (step, down)]
        if step % 2:
            odd[-step], odd[step] = up, down
    place = ring_place(lax.axis_index("row"), n)
    wanted = (half - 2 * place - 1 + half - 1 + 4 * n) % n - (half - 1)
    send = odd[1]
    for distance, block in odd.items():
        if distance != 1:
            send = jnp.where(wanted == distance, block, send)
    other = lax.ppermute(send, "row", [(i, i ^ 1) for i in range(n)])
    return found + [(half, other)]


def per_device(ladder_ints, amplitudes, phase_map):
    n = lax.axis_size("row")
    cols = lax.axis_size("col")
    rows = amplitudes.shape[0] // cols
    width = amplitudes.shape[1]
    group = TILE // n
    tiles = -(-rows // group)
    padded = tiles * group
    half = width // 2

    def partner(j):
        return [(i, i ^ j) for i in range(cols)]

    pieces = cut(amplitudes, cols, rows, padded)
    high, low = order(ladder_ints, n, tiles)

    def swap(x, j):
        return lax.ppermute(x, "col", partner(j))

    ranks = sorted(range(1, cols), key=lambda j: (-bin(j).count("1"), j))
    arrived = {j: swap(pieces[j], j) for j in ranks}

    far = [j for j in ranks if bin(j).count("1") > 1]
    near = [j for j in ranks if bin(j).count("1") == 1]
    chunks = [[(j, 0), (j, 1)] for j in far]
    for a in range(0, len(near), 2):
        pair = near[a : a + 2]
        if len(pair) == 2:
            chunks += [[(pair[0], h), (pair[1], h)] for h in (0, 1)]
        else:
            chunks += [[(pair[0], 0), (pair[0], 1)]]
    waiting = {(j, h): [] for j in range(cols) for h in (0, 1)}

    def multiply(chunk, adds, outs):
        found = gather(chunk, n)
        offsets = tuple(d for d, _ in found)
        return product(
            phase_map, high, low, [b for _, b in found], offsets, tiles, adds, outs
        )

    for chunk in chunks:
        if chunk[0][0] == chunk[1][0]:
            block = arrived[chunk[0][0]]
        else:
            block = jnp.concatenate(
                [arrived[j][:, h * half : (h + 1) * half] for j, h in chunk], axis=1
            )
        adds = [(a, i * half) for i, key in enumerate(chunk) for a in waiting[key]]
        sums = multiply(block, adds, ((0, half), (half, half)))
        for (j, h), value in zip(chunk, sums):
            bits = [1 << b for b in range(cols) if j >> b & 1]
            bit = bits[0] if h == 0 else bits[-1]
            waiting[j ^ bit, h].append(swap(value, bit))

    adds = [(a, h * half) for h in (0, 1) for a in waiting[0, h]]
    return multiply(pieces[0], adds, ((0, width),))[0]


def solution(mesh):
    in_specs = (P("row", "col"), P("row", "col"), P())
    out_specs = P("row", "col")
    return jax.shard_map(
        per_device, mesh=mesh, in_specs=in_specs, out_specs=out_specs, check_vma=False
    )
```

```python
import functools

import jax
import jax.numpy as jnp
from jax import lax
from jax.experimental import pallas as pl
from jax.experimental.pallas import tpu as pltpu
from jax.sharding import PartitionSpec as P

TILE = 256


def ring_row(position, n):
    return jnp.where(position < n // 2, 2 * position, 2 * (n - 1 - position) + 1)


def ring_place(row, n):
    return jnp.where(row % 2 == 0, row // 2, n - 1 - row // 2)


def room(*arrays):
    total = sum(a.size * a.dtype.itemsize for a in arrays)
    return pltpu.CompilerParams(vmem_limit_bytes=total + total // 4 + (2 << 20))


def ring_pairs(n):
    order = list(range(0, n, 2)) + list(range(n - 1, 0, -2))
    forward = [(order[i], order[(i + 1) % n]) for i in range(n)]
    return forward, [(b, a) for a, b in forward]


def split(x):
    high = x.astype(jnp.bfloat16)
    low = (x - high.astype(jnp.float32)).astype(jnp.bfloat16)
    return high, low


def cut_kernel(cols, rows, source, *pieces):
    me = lax.axis_index("col")
    for piece in pieces:
        piece[rows:, :] = jnp.zeros((piece.shape[0] - rows, piece.shape[1]), jnp.float32)
    for own in range(cols):

        @pl.when(me == own)
        def _():
            for j, piece in enumerate(pieces):
                start = (own ^ j) * rows
                piece[:rows, :] = source[start : start + rows, :]


def cut(amplitudes, cols, rows, padded):
    width = amplitudes.shape[1]
    out = jax.ShapeDtypeStruct((padded, width), jnp.float32)
    return pl.pallas_call(
        functools.partial(cut_kernel, cols, rows),
        out_shape=[out] * cols,
        name="cut",
        compiler_params=room(amplitudes, *[out] * cols),
        cost_estimate=pl.CostEstimate(
            flops=amplitudes.size, bytes_accessed=8 * amplitudes.size, transcendentals=0
        ),
    )(amplitudes)


def order_kernel(phases, tiles, ints, high_out, low_out):
    group = TILE // phases
    into = lax.broadcasted_iota(jnp.int32, (TILE, TILE), 1)
    source = lax.broadcasted_iota(jnp.int32, (TILE, TILE), 0)
    wanted = (into % group) * phases + into // group
    pick = jnp.where(source == wanted, 1.0, 0.0).astype(jnp.bfloat16)
    total = ints.shape[1]
    for t in range(tiles):
        stop = min(TILE, total - t * TILE)
        high, low = split(ints[:, t * TILE : t * TILE + stop])
        chosen = pick[:stop, :]
        at = pl.ds(t * TILE, TILE)
        high_out[:, at] = jnp.dot(
            high, chosen, preferred_element_type=jnp.float32
        ).astype(jnp.bfloat16)
        low_out[:, at] = jnp.dot(
            low, chosen, preferred_element_type=jnp.float32
        ).astype(jnp.bfloat16)


def order(ints, phases, tiles):
    out = jax.ShapeDtypeStruct((ints.shape[0], tiles * TILE), jnp.bfloat16)
    return pl.pallas_call(
        functools.partial(order_kernel, phases, tiles),
        out_shape=[out, out],
        name="order",
        compiler_params=room(ints, out, out),
        cost_estimate=pl.CostEstimate(
            flops=4 * ints.size * TILE, bytes_accessed=8 * ints.size, transcendentals=0
        ),
    )(ints)


def product_kernel(offsets, tiles, n_add, outs, phase_map, high, low, *refs):
    blocks = refs[: len(offsets)]
    adds = refs[len(offsets) : len(offsets) + len(n_add)]
    results = refs[len(offsets) + len(n_add) : len(offsets) + len(n_add) + len(outs)]
    t_high, t_low = refs[-2:]
    n = len(offsets)
    group = TILE // n
    place = ring_place(lax.axis_index("row"), n)
    for block, offset in zip(blocks, offsets):
        phase = phase_map[ring_row((place + offset + n) % n, n)]
        b_high, b_low = split(block[...])
        for t in range(tiles):
            at = pl.ds(pl.multiple_of(t * TILE + phase * group, group), group)
            t_high[at, :] = b_high[t * group : (t + 1) * group, :]
            t_low[at, :] = b_low[t * group : (t + 1) * group, :]
    total = jnp.dot(high[...], t_high[...], preferred_element_type=jnp.float32)
    total += jnp.dot(low[...], t_high[...], preferred_element_type=jnp.float32)
    total += jnp.dot(high[...], t_low[...], preferred_element_type=jnp.float32)
    parts = {}
    for result, (start, width) in zip(results, outs):
        value = total[:, start : start + width]
        for add, (first, size) in zip(adds, n_add):
            if first == start and size == width:
                value += add[...]
            elif start <= first and first + size <= start + width:
                parts.setdefault((start, width), []).append((add, first - start, size))
        result[...] = value
        for add, first, size in parts.get((start, width), []):
            result[:, first : first + size] += add[...]


def product(phase_map, high, low, blocks, offsets, tiles, adds, outs):
    rows, depth = high.shape
    width = blocks[0].shape[1]
    vmem = pl.BlockSpec(memory_space=pltpu.VMEM)
    spots = tuple((first, a.shape[1]) for a, first in adds)
    results = [jax.ShapeDtypeStruct((rows, w), jnp.float32) for _, w in outs]
    held = jax.ShapeDtypeStruct((depth, width), jnp.float32)
    return pl.pallas_call(
        functools.partial(product_kernel, offsets, tiles, spots, outs),
        out_shape=results,
        in_specs=[pl.BlockSpec(memory_space=pltpu.SMEM)] + [vmem] * (2 + len(blocks) + len(adds)),
        scratch_shapes=[pltpu.VMEM((depth, width), jnp.bfloat16)] * 2,
        name="product",
        compiler_params=room(high, low, *blocks, *[a for a, _ in adds], *results, held),
        cost_estimate=pl.CostEstimate(
            flops=6 * rows * depth * width,
            bytes_accessed=4 * rows * depth + 4 * depth * width + 4 * rows * width,
            transcendentals=0,
        ),
    )(phase_map, high, low, *blocks, *[a for a, _ in adds])


def gather(chunk, n):
    forward, backward = ring_pairs(n)
    half = n // 2
    up, down = chunk, chunk
    found = [(0, chunk)]
    odd = {}
    for step in range(1, half):
        up = lax.ppermute(up, "row", forward)
        down = lax.ppermute(down, "row", backward)
        found += [(-step, up), (step, down)]
        if step % 2:
            odd[-step], odd[step] = up, down
    place = ring_place(lax.axis_index("row"), n)
    wanted = (half - 2 * place - 1 + half - 1 + 4 * n) % n - (half - 1)
    send = odd[1]
    for distance, block in odd.items():
        if distance != 1:
            send = jnp.where(wanted == distance, block, send)
    other = lax.ppermute(send, "row", [(i, i ^ 1) for i in range(n)])
    return found + [(half, other)]


def per_device(ladder_ints, amplitudes, phase_map):
    n = lax.axis_size("row")
    cols = lax.axis_size("col")
    rows = amplitudes.shape[0] // cols
    width = amplitudes.shape[1]
    group = TILE // n
    tiles = -(-rows // group)
    padded = tiles * group
    half = width // 2

    def partner(j):
        return [(i, i ^ j) for i in range(cols)]

    pieces = cut(amplitudes, cols, rows, padded)
    high, low = order(ladder_ints, n, tiles)

    def swap(x, j):
        return lax.ppermute(x, "col", partner(j))

    ranks = sorted(range(1, cols), key=lambda j: (-bin(j).count("1"), j))
    arrived = {j: swap(pieces[j], j) for j in ranks}

    far = [j for j in ranks if bin(j).count("1") > 1]
    near = [j for j in ranks if bin(j).count("1") == 1]
    chunks = [[(j, 0), (j, 1)] for j in far]
    for a in range(0, len(near), 2):
        pair = near[a : a + 2]
        if len(pair) == 2:
            chunks += [[(pair[0], h), (pair[1], h)] for h in (0, 1)]
        else:
            chunks += [[(pair[0], 0), (pair[0], 1)]]
    waiting = {(j, h): [] for j in range(cols) for h in (0, 1)}

    def multiply(chunk, adds, outs):
        found = gather(chunk, n)
        offsets = tuple(d for d, _ in found)
        return product(
            phase_map, high, low, [b for _, b in found], offsets, tiles, adds, outs
        )

    for chunk in chunks:
        if chunk[0][0] == chunk[1][0]:
            block = arrived[chunk[0][0]]
        else:
            block = jnp.concatenate(
                [arrived[j][:, h * half : (h + 1) * half] for j, h in chunk], axis=1
            )
        adds = [(a, i * half) for i, key in enumerate(chunk) for a in waiting[key]]
        sums = multiply(block, adds, ((0, half), (half, half)))
        for (j, h), value in zip(chunk, sums):
            bits = [1 << b for b in range(cols) if j >> b & 1]
            bit = bits[0] if h == 0 else bits[-1]
            waiting[j ^ bit, h].append(swap(value, bit))

    adds = [(a, h * half) for h in (0, 1) for a in waiting[0, h]]
    return multiply(pieces[0], adds, ((0, width),))[0]


def solution(mesh):
    in_specs = (P("row", "col"), P("row", "col"), P())
    out_specs = P("row", "col")
    return jax.shard_map(
        per_device, mesh=mesh, in_specs=in_specs, out_specs=out_specs, check_vma=False
    )
```
